32 devices in a mesh: outer: 4 (over z), inner: 8 (over y, x, core).
Axes of the slice: x: 2, y: 2, z: 4, core: 2. Of those that a mesh axis runs over, the one named last changes fastest.
Arguments:
- query_proj: bfloat16 [2048, 8192], P(('outer', 'inner')), may hold values from -8 to 8
- key_proj: bfloat16 [2048, 512], P(('outer', 'inner')), may hold values from -8 to 8
- value_proj: bfloat16 [2048, 512], P(('outer', 'inner')), may hold values from -6 to 6
- positions: int32 [2048], P(('outer', 'inner')), may hold values from 0 to 2047, each once
Outputs:
- attended: bfloat16 [2048, 8192], P(('outer', 'inner'))
The draws below stay inside these ranges and needn't reach their ends.
Inputs may be any that keep to these rules, and one draw needn't show every extreme that they name: `positions`: each position from 0 to 2047 appears exactly once.
All inputs are finite; a program needn't handle non-finite values.
Results may differ from the reference program's by a relative error of at most 0.005.
Values may be sent and summed in bfloat16 or wider, within the bound.
A program may use at most 64 MiB of HBM per device.

```python
import math
import jax
import jax.numpy as jnp
from jax import lax

HEADS = 64
KV_HEADS = 4
HEAD_WIDTH = 128
TOKENS = 2048


def draw_query_proj(key, part):
    shape_rows = TOKENS
    width = HEADS * HEAD_WIDTH
    sub_key = jax.random.fold_in(key, 1)
    base = 1.4 * jax.random.normal(sub_key, (shape_rows, width), jnp.float32)
    return jnp.clip(base, -8.0, 8.0).astype(jnp.bfloat16)


def draw_key_proj(key, part):
    shape_rows = TOKENS
    width = KV_HEADS * HEAD_WIDTH
    sub_key = jax.random.fold_in(key, 2)
    base = 1.4 * jax.random.normal(sub_key, (shape_rows, width), jnp.float32)
    return jnp.clip(base, -8.0, 8.0).astype(jnp.bfloat16)


def block_levels(stream_key, shape, shards, low, high):
    factor_of, own = 1.0, jax.random.fold_in(stream_key, 6)
    for axis_at, blocks in shards:
        heights = jnp.exp(jax.random.uniform(jax.random.fold_in(own, axis_at), (blocks,), jnp.float32, low / len(shards), high / len(shards)))
        factor_of = factor_of * jnp.repeat(heights, shape[axis_at] // blocks).reshape([-1 if axis == axis_at else 1 for axis in range(len(shape))])
    return factor_of


def gaussian(key, dims, scale, bound, shards=(), kind=jnp.bfloat16):
    array = scale * jax.random.normal(key, dims, jnp.float32)
    if shards:
        array = array * block_levels(key, dims, shards, -0.22, 0.18)
    return jnp.clip(array, -bound, bound).astype(kind)


def setup_inputs(seed: int = 0) -> dict:
    key_of = jax.random.split(jax.random.key(seed), 5)
    return {
        "query_proj": draw_query_proj(jax.random.fold_in(key_of[4], 71), 0),
        "key_proj": draw_key_proj(jax.random.fold_in(key_of[4], 71), 0),
        "value_proj": gaussian(key_of[2], (TOKENS, KV_HEADS * HEAD_WIDTH), 1.0, 6.0, ((0, 32),)),
        "positions": jax.random.permutation(key_of[3], TOKENS).astype(jnp.int32),
    }


def reference(query_proj, key_proj, value_proj, positions):
    all_tokens = query_proj.shape[0]
    group_size = HEADS // KV_HEADS
    scaling = 1.0 / math.sqrt(HEAD_WIDTH)
    query_view = query_proj.reshape(all_tokens, KV_HEADS, group_size, HEAD_WIDTH)
    key_heads = key_proj.reshape(all_tokens, KV_HEADS, HEAD_WIDTH).transpose(1, 0, 2).astype(jnp.float32)
    value_heads = value_proj.reshape(all_tokens, KV_HEADS, HEAD_WIDTH).transpose(1, 0, 2).astype(jnp.float32)
    block_rows = math.gcd(all_tokens, 512)
    block_count = all_tokens // block_rows

    def one_block(block_index):
        first_row = (block_index * block_rows).astype(jnp.int32)
        query_block = lax.dynamic_slice_in_dim(query_view, first_row, block_rows, 0).astype(jnp.float32)
        query_pos = lax.dynamic_slice_in_dim(positions, first_row, block_rows, 0)
        visible = positions[None, :] <= query_pos[:, None]

        def one_head(operands):
            query_head, key_head, value_head = operands
            scores = jnp.einsum('qgd,kd->gqk', query_head, key_head) * scaling
            row_top = lax.optimization_barrier(jnp.max(jnp.where(visible[None], scores, -1e+30), axis=2))
            softmax_weights = jnp.where(visible[None], jnp.exp(scores - row_top[:, :, None]), 0.0)
            row_total_sum = lax.optimization_barrier(jnp.sum(softmax_weights, axis=2))
            rounded = softmax_weights.astype(jnp.bfloat16).astype(jnp.float32)
            weighted = jnp.einsum('gqk,kd->gqd', rounded, value_head)
            return weighted / row_total_sum[:, :, None]
        outputs = lax.map(one_head, (query_block.transpose(1, 0, 2, 3), key_heads, value_heads))
        return outputs.transpose(2, 0, 1, 3).reshape(block_rows, HEADS * HEAD_WIDTH).astype(jnp.bfloat16)
    blocks = lax.map(one_block, jnp.arange(block_count, dtype=jnp.int32))
    return blocks.reshape(all_tokens, HEADS * HEAD_WIDTH)
```

```python
import functools
import math

import jax
import jax.numpy as jnp
from jax import lax
from jax.experimental import pallas as pl
from jax.experimental.pallas import tpu as pltpu
from jax.sharding import PartitionSpec as P

HEAD_WIDTH = 128
HIDDEN = -1e30
POS = 2
KINDS = (POS, 0, 1)
MESH = pl.DeviceIdType.MESH


def rank_of(p, s, nz):
    d = jnp.abs(s - p)
    m = jnp.minimum(p, nz - 1 - p)
    return jnp.where(d <= m, 2 * d - jnp.where(s < p, 1, 0), m + d)


def source_of(p, n, nz):
    m = jnp.minimum(p, nz - 1 - p)
    near = n <= 2 * m
    d = jnp.where(near, (n + 1) // 2, n - m)
    below = jnp.where(near, n % 2, jnp.where(p > nz - 1 - p, 1, 0))
    return p + d * (1 - 2 * below)


def kernel(sizes, q_ref, k_ref, v_ref, pos_ref, out_ref, buf, pbuf, other, mask, top, acc,
           q_buf, o_buf, copy_sem, recv_sem, q_sem, out_sem, send_sem):
    nz, ny, nx, rows, kinds, group = sizes
    d = HEAD_WIDTH
    chips = ny * nx
    both = 2 * rows
    keys = chips * both
    half = kinds * group * d
    z = lax.axis_index("outer")
    inner = lax.axis_index("inner")
    core = lax.rem(inner, 2)
    x = lax.rem(inner // 2, nx)
    y = inner // (2 * nx)

    def plane(dy=0, dx=0, dc=0, zz=None):
        yy = lax.rem(y + dy, ny)
        xx = lax.rem(x + dx, nx)
        cc = lax.rem(core + dc, 2)
        return (z if zz is None else zz, (yy * nx + xx) * 2 + cc)

    def slot(dx, dy):
        return dy * nx + dx

    local = []

    def fetch(src, dst):
        c = pltpu.make_async_copy(src, dst, copy_sem.at[len(local)])
        c.start()
        local.append(c)

    def head_cols(c, kind):
        return pl.ds(pl.multiple_of((c * kinds + kind) * d, d), d)

    for kind in range(kinds):
        for part, ref in enumerate((k_ref, v_ref)):
            cols = pl.ds(part * d, d)
            fetch(ref.at[:, head_cols(core, kind)], buf.at[0, kind, 0, pl.ds(0, rows), cols])
            fetch(ref.at[:, head_cols(1 - core, kind)], other.at[kind, :, cols])
    fetch(pos_ref, pbuf.at[0, 0, 0])
    early = len(local)
    my_cols = pl.ds(pl.multiple_of(core * half, half), half)
    their_cols = pl.ds(pl.multiple_of((1 - core) * half, half), half)
    fetch(q_ref.at[:, my_cols], q_buf.at[pl.ds(0, rows)])

    up, down = z + 1 < nz, z > 0
    barrier = pltpu.get_barrier_semaphore()

    def greet(where):
        pl.semaphore_signal(barrier, inc=1, device_id=where, device_id_type=MESH)

    fixed = 1
    greet(plane(dc=1))
    for dc in range(2):
        for dx in range(1, nx):
            greet(plane(dx=dx, dc=dc))
            fixed += 1
        for dy in range(1, ny):
            greet(plane(dy=dy, dc=dc))
            fixed += 1
        pl.when(up)(functools.partial(greet, plane(dc=dc, zz=z + 1)))
        pl.when(down)(functools.partial(greet, plane(dc=dc, zz=z - 1)))
    pl.semaphore_wait(barrier, fixed + 2 * (jnp.where(up, 1, 0) + jnp.where(down, 1, 0)))
    for c in local[:early]:
        c.wait()

    sent = []

    def ref_of(n, kind, sl, piece=None):
        if kind == POS:
            r = pbuf.at[n, sl]
            return r if piece is None else r.at[piece]
        r = buf.at[n, kind, sl]
        return r if piece is None else r.at[pl.ds(piece * rows, rows)]

    def send(src, dst, sem, to, when=None):
        c = pltpu.make_async_remote_copy(
            src_ref=src, dst_ref=dst, send_sem=send_sem.at[len(sent)], recv_sem=sem,
            device_id=to, device_id_type=MESH)
        sent.append((c, when))
        if when is None:
            c.start()
        else:
            pl.when(when)(c.start)

    def arrived(n, kind, sl):
        r = ref_of(n, kind, sl, None if n or sl else 1)
        pltpu.make_async_remote_copy(
            src_ref=r, dst_ref=r, send_sem=send_sem.at[0], recv_sem=recv_sem.at[n, kind, sl],
            device_id=plane(dc=1), device_id_type=MESH).wait_recv()

    def send_own(kind, n, sl, when=None, **to):
        send(ref_of(0, kind, 0, 0), ref_of(n, kind, sl, 0), recv_sem.at[n, kind, sl],
             plane(**to), when)
        mine = pbuf.at[0, 0, 0] if kind == POS else other.at[kind]
        send(mine, ref_of(n, kind, sl, 1), recv_sem.at[n, kind, sl], plane(dc=1, **to), when)

    def pass_on(kind, n, here, n_there, there, when=None, **to):
        send(ref_of(n, kind, here), ref_of(n_there, kind, there),
             recv_sem.at[n_there, kind, there], plane(**to), when)

    for kind in KINDS:
        mine = pbuf.at[0, 0, 0] if kind == POS else other.at[kind]
        send_own(kind, rank_of(z + 1, z, nz), 0, when=up, zz=z + 1)
        send_own(kind, rank_of(z - 1, z, nz), 0, when=down, zz=z - 1)
        for dx in range(1, nx):
            send_own(kind, 0, slot(dx, 0), dx=dx)
        for dy in range(1, ny):
            send_own(kind, 0, slot(0, dy), dy=dy)
        send(mine, ref_of(0, kind, 0, 1), recv_sem.at[0, kind, 0], plane(dc=1))
    send(q_ref.at[:, their_cols], q_buf.at[pl.ds(rows, rows)], q_sem, plane(dc=1))

    def along(n, kinds_now):
        source = source_of(z, n, nz)
        step = jnp.where(source < z, 1, -1)
        there = z + step
        more = jnp.logical_and(there >= 0, there < nz)
        for kind in kinds_now:
            pl.when(more)(functools.partial(arrived, n, kind, 0))
            pass_on(kind, n, 0, rank_of(there, source, nz), 0, when=more, zz=there)

    def across(n, kinds_now):
        source = source_of(z, n, nz)
        there = z + jnp.where(source < z, 1, -1)
        last = jnp.logical_or(there < 0, there >= nz)
        for kind in kinds_now:
            pl.when(last)(functools.partial(arrived, n, kind, 0))
            for dx in range(1, nx):
                pass_on(kind, n, 0, n, slot(dx, 0), dx=dx)
            for dy in range(1, ny):
                pass_on(kind, n, 0, n, slot(0, dy), dy=dy)

    def relay(n, kinds_now):
        for kind in kinds_now:
            if kind == 1:
                for dy in range(1, ny):
                    arrived(n, kind, slot(0, dy))
                    for dx in range(1, nx):
                        pass_on(kind, n, slot(0, dy), n, slot(dx, dy), dx=dx)
            else:
                for dx in range(1, nx):
                    arrived(n, kind, slot(dx, 0))
                    for dy in range(1, ny):
                        pass_on(kind, n, slot(dx, 0), n, slot(dx, dy), dy=dy)

    def gather(n, kinds_now):
        for kind in kinds_now:
            if n == 0:
                arrived(0, kind, 0)
            for dy in range(1, ny):
                if kind != 1:
                    arrived(n, kind, slot(0, dy))
            for dx in range(1, nx):
                if kind == 1:
                    arrived(n, kind, slot(dx, 0))
                for dy in range(1, ny):
                    arrived(n, kind, slot(dx, dy))

    def positions_of(n, sl):
        return jnp.concatenate([pbuf[n, sl, 0], pbuf[n, sl, 1]], axis=1).astype(jnp.float32)

    def build_mask(n):
        mine = jnp.broadcast_to(positions_of(0, 0), (both, both))
        for sl in range(chips):
            theirs = jnp.broadcast_to(positions_of(n, sl), (both, both)).T
            mask[n, sl * both:(sl + 1) * both, :] = jnp.where(
                theirs > mine, HIDDEN, 0.0).astype(jnp.bfloat16)

    eye = (lax.broadcasted_iota(jnp.int32, (both, both), 0)
           == lax.broadcasted_iota(jnp.int32, (both, both), 1)).astype(jnp.bfloat16)
    scale = math.log2(math.e) / math.sqrt(d)
    per_tile = math.gcd(max(1, 512 // both), group)
    tile = per_tile * both
    tiles = group // per_tile
    ones = jnp.ones((keys, d), jnp.bfloat16)

    def compute(n, kind):
        k_wide = jnp.concatenate([buf[n, kind, :, :, :d].reshape(keys, d), mask[n]], axis=1)
        v_wide = jnp.concatenate([buf[n, kind, :, :, d:].reshape(keys, d), ones], axis=1)

        def columns(t, j):
            at = (kind * group + t * per_tile + j) * d
            return slice(at, at + d)

        def score(t):
            query = jnp.concatenate(
                [jnp.concatenate([q_buf[:, columns(t, j)], eye], axis=1)
                 for j in range(per_tile)], axis=0)
            return lax.dot_general(query, k_wide, (((1,), (1,)), ((), ())),
                                   preferred_element_type=jnp.float32)

        def fold(t, scores):
            window = slice(t * tile, (t + 1) * tile)
            new_top = jnp.broadcast_to(jnp.max(scores, axis=1, keepdims=True), (tile, d))
            if n:
                old_top = top[kind, window, :]
                new_top = jnp.maximum(old_top, new_top)
                rescale = jnp.exp2((old_top - new_top) * scale)
            weights = jnp.exp2((scores - jnp.concatenate([new_top] * (keys // d), axis=1))
                               * scale).astype(jnp.bfloat16)
            got = lax.dot_general(weights, v_wide, (((1,), (0,)), ((), ())),
                                  preferred_element_type=jnp.float32)
            if n:
                got = acc[kind, window, :] * jnp.concatenate([rescale, rescale], axis=1) + got
            if n < nz - 1:
                acc[kind, window, :] = got
                top[kind, window, :] = new_top
                return
            result = (got[:, :d] / got[:, d:]).astype(jnp.bfloat16)
            for j in range(per_tile):
                o_buf[:, columns(t, j)] = result[j * both + rows:(j + 1) * both, :]
            for j in range(per_tile):
                at = columns(t, j).start
                out_ref[:, pl.ds(pl.multiple_of(core * half + at, d), d)] = (
                    result[j * both:j * both + rows, :])

        held = score(0)
        for t in range(tiles):
            following = score(t + 1) if t + 1 < tiles else None
            fold(t, held)
            held = following
        if n == nz - 1:
            wide = group * d
            send(o_buf.at[:, pl.ds(kind * wide, wide)],
                 out_ref.at[:, pl.ds(pl.multiple_of(core * half + kind * wide, wide), wide)],
                 out_sem.at[kind], plane(dc=1))

    first, second = (POS, 0), (1,)
    todo = [(n, ks) for n in range(nz) for ks in (first, second)]

    def ahead(i, what):
        if i < len(todo) and todo[i][0] > 0:
            what(*todo[i])

    def relay_at(i):
        if 0 <= i < len(todo):
            relay(*todo[i])

    ahead(2, along)
    ahead(4, along)
    ahead(2, across)
    relay_at(0)
    ahead(3, along)
    ahead(5, along)
    ahead(3, across)
    relay_at(1)
    ahead(6, along)
    ahead(4, across)
    relay_at(2)
    local[early].wait()
    pltpu.make_async_remote_copy(
        src_ref=q_buf.at[pl.ds(rows, rows)], dst_ref=q_buf.at[pl.ds(rows, rows)],
        send_sem=send_sem.at[0], recv_sem=q_sem, device_id=plane(dc=1),
        device_id_type=MESH).wait_recv()
    for i, (n, ks) in enumerate(todo):
        gather(n, ks)
        if POS in ks:
            build_mask(n)
        compute(n, ks[-1])
        ahead(i + 7, along)
        ahead(i + 5, across)
        relay_at(i + 3)
    wide = group * d
    for kind in range(kinds):
        r = out_ref.at[:, pl.ds(pl.multiple_of((1 - core) * half + kind * wide, wide), wide)]
        pltpu.make_async_remote_copy(
            src_ref=r, dst_ref=r, send_sem=send_sem.at[0], recv_sem=out_sem.at[kind],
            device_id=plane(dc=1), device_id_type=MESH).wait_recv()
    for c, when in sent:
        if when is None:
            c.wait_send()
        else:
            pl.when(when)(c.wait_send)


def body(query_proj, key_proj, value_proj, positions):
    rows, width = query_proj.shape
    d = HEAD_WIDTH
    heads_kv = key_proj.shape[1] // d
    group = width // d // heads_kv
    nz = lax.axis_size("outer")
    inner = lax.axis_size("inner")
    nx = 2
    ny = inner // (2 * nx)
    chips = ny * nx
    kinds = heads_kv // 2
    both = 2 * rows
    sizes = (nz, ny, nx, rows, kinds, group)
    near = nx - 1 + ny - 1
    copies = (6 * (near + 2) + 4 + 3 * (nz - 1) * (1 + near)
              + 3 * nz * (nx - 1) * (ny - 1) + kinds)
    hbm = pl.BlockSpec(memory_space=pltpu.HBM)
    operands = [pltpu.with_memory_space_constraint(a, pltpu.HBM) for a in (
        query_proj, key_proj, value_proj, positions.reshape(1, rows))]
    return pl.pallas_call(
        functools.partial(kernel, sizes),
        out_shape=pltpu.VMEM((rows, width), jnp.bfloat16),
        in_specs=[hbm, hbm, hbm, hbm],
        out_specs=pl.BlockSpec(memory_space=pltpu.VMEM),
        scratch_shapes=[
            pltpu.VMEM((nz, kinds, chips, both, 2 * d), jnp.bfloat16),
            pltpu.VMEM((nz, chips, 2, 1, rows), jnp.int32),
            pltpu.VMEM((kinds, rows, 2 * d), jnp.bfloat16),
            pltpu.VMEM((nz, chips * both, both), jnp.bfloat16),
            pltpu.VMEM((kinds, group * both, d), jnp.float32),
            pltpu.VMEM((kinds, group * both, 2 * d), jnp.float32),
            pltpu.VMEM((both, width // 2), jnp.bfloat16),
            pltpu.VMEM((rows, width // 2), jnp.bfloat16),
            pltpu.SemaphoreType.DMA((4 * kinds + 2,)),
            pltpu.SemaphoreType.DMA((nz, 3, chips)),
            pltpu.SemaphoreType.DMA,
            pltpu.SemaphoreType.DMA((kinds,)),
            pltpu.SemaphoreType.DMA((copies,)),
        ],
        compiler_params=pltpu.CompilerParams(
            collective_id=0, has_side_effects=True, vmem_limit_bytes=48 * 1024 * 1024),
    )(*operands)


def solution(mesh):
    return jax.shard_map(
        body,
        mesh=mesh,
        in_specs=(
            P(("outer", "inner"), None),
            P(("outer", "inner"), None),
            P(("outer", "inner"), None),
            P(("outer", "inner")),
        ),
        out_specs=P(("outer", "inner"), None),
        check_vma=False,
    )
```

```python
import functools
import math

import jax
import jax.numpy as jnp
from jax import lax
from jax.experimental import pallas as pl
from jax.experimental.pallas import tpu as pltpu
from jax.sharding import PartitionSpec as P

HEAD_WIDTH = 128
HIDDEN = -1e30
PIECES = 4
POS = PIECES
MESH = pl.DeviceIdType.MESH


def rank_of(p, s, nz):
    d = jnp.abs(s - p)
    m = jnp.minimum(p, nz - 1 - p)
    return jnp.where(d <= m, 2 * d - jnp.where(s < p, 1, 0), m + d)


def source_of(p, n, nz):
    m = jnp.minimum(p, nz - 1 - p)
    near = n <= 2 * m
    d = jnp.where(near, (n + 1) // 2, n - m)
    below = jnp.where(near, n % 2, jnp.where(p > nz - 1 - p, 1, 0))
    return p + d * (1 - 2 * below)


def kernel(sizes, q_ref, k_ref, v_ref, pos_ref, out_ref, buf, pbuf, other, mask, top, acc,
           q_buf, o_buf, copy_sem, recv_sem, q_sem, out_sem, send_sem):
    nz, ny, nx, rows, kinds, group = sizes
    d = HEAD_WIDTH
    chips = ny * nx
    both = 2 * rows
    keys = chips * both
    half = kinds * group * d
    z = lax.axis_index("outer")
    inner = lax.axis_index("inner")
    core = lax.rem(inner, 2)
    x = lax.rem(inner // 2, nx)
    y = inner // (2 * nx)

    def plane(dy=0, dx=0, dc=0, zz=None):
        yy = lax.rem(y + dy, ny)
        xx = lax.rem(x + dx, nx)
        cc = lax.rem(core + dc, 2)
        return (z if zz is None else zz, (yy * nx + xx) * 2 + cc)

    def slot(dx, dy):
        return dy * nx + dx

    def fetch(src, dst, n):
        c = pltpu.make_async_copy(src, dst, copy_sem.at[n])
        c.start()
        return c

    def head_cols(c, kind):
        return pl.ds(pl.multiple_of((c * kinds + kind) * d, d), d)

    for piece in range(PIECES):
        ref = v_ref if piece % 2 else k_ref
        fetch(ref.at[:, head_cols(core, piece // 2)], buf.at[0, piece, 0, pl.ds(0, rows)], 0)
        fetch(ref.at[:, head_cols(1 - core, piece // 2)], other.at[piece], 0)
    pos_copy = fetch(pos_ref, pbuf.at[0, 0, 0], 1)
    my_cols = pl.ds(pl.multiple_of(core * half, half), half)
    their_cols = pl.ds(pl.multiple_of((1 - core) * half, half), half)
    q_copy = fetch(q_ref.at[:, my_cols], q_buf.at[pl.ds(0, rows)], 2)

    up, down = z + 1 < nz, z > 0
    barrier = pltpu.get_barrier_semaphore()

    def greet(where):
        pl.semaphore_signal(barrier, inc=1, device_id=where, device_id_type=MESH)

    fixed = 1
    greet(plane(dc=1))
    for dc in range(2):
        for dx in range(1, nx):
            greet(plane(dx=dx, dc=dc))
            fixed += 1
        for dy in range(1, ny):
            greet(plane(dy=dy, dc=dc))
            fixed += 1
        pl.when(up)(functools.partial(greet, plane(dc=dc, zz=z + 1)))
        pl.when(down)(functools.partial(greet, plane(dc=dc, zz=z - 1)))
    pl.semaphore_wait(barrier, fixed + 2 * (jnp.where(up, 1, 0) + jnp.where(down, 1, 0)))
    pos_copy.wait()
    pltpu.make_async_copy(buf.at[0, :, 0], buf.at[0, :, 0], copy_sem.at[0]).wait()

    groups = {}
    waited = set()
    half_way = min(2, nz - 1)

    def on_line(n, piece):
        return piece == PIECES - 1 and 0 < n <= half_way

    def x_first(n, piece):
        return (n + piece) % 2 == 0

    def ref_of(n, piece, sl, part=None):
        if piece == POS:
            r = pbuf.at[n, sl]
            return r if part is None else r.at[part]
        r = buf.at[n, piece, sl]
        return r if part is None else r.at[pl.ds(part * rows, rows)]

    def send(src, dst, sem, to, group, when=None):
        at, cond, copies = groups.setdefault(group, (len(groups), when, []))
        c = pltpu.make_async_remote_copy(
            src_ref=src, dst_ref=dst, send_sem=send_sem.at[at], recv_sem=sem,
            device_id=to, device_id_type=MESH)
        copies.append(math.prod(src.shape))
        if when is None:
            c.start()
        else:
            pl.when(when)(c.start)

    def all_sent():
        for (is_pos, *_), (at, cond, copies) in groups.items():
            lines = sum(copies) // (rows if is_pos else rows * d)
            if is_pos:
                r = pbuf.at[0, pl.ds(0, lines // 2)] if lines > 1 else pbuf.at[0, 0, 0]
            else:
                r = q_buf.at[pl.ds(0, rows), pl.ds(0, lines * d)]
            c = pltpu.make_async_remote_copy(
                src_ref=r, dst_ref=r, send_sem=send_sem.at[at], recv_sem=q_sem,
                device_id=plane(dc=1), device_id_type=MESH)
            if cond is None:
                c.wait_send()
            else:
                pl.when(cond)(c.wait_send)

    def landed(r, sem):
        pltpu.make_async_remote_copy(
            src_ref=r, dst_ref=r, send_sem=send_sem.at[0], recv_sem=sem,
            device_id=plane(dc=1), device_id_type=MESH).wait_recv()

    def arrived(n, piece, sl):
        if (n, piece, sl) not in waited:
            waited.add((n, piece, sl))
            landed(ref_of(n, piece, sl, 1 if n == sl == 0 else None), recv_sem.at[n, piece, sl])

    def arrived_if(when, n, piece, sl):
        pl.when(when)(lambda: landed(ref_of(n, piece, sl), recv_sem.at[n, piece, sl]))

    def pass_on(name, n, piece, here, there, n_there=None, when=None, **to):
        n_there = n if n_there is None else n_there
        send(ref_of(n, piece, here), ref_of(n_there, piece, there),
             recv_sem.at[n_there, piece, there], plane(**to), (piece == POS, name, n), when)

    def send_own(name, piece, n, sl, when=None, **to):
        group = (piece == POS, name)
        send(ref_of(0, piece, 0, 0), ref_of(n, piece, sl, 0), recv_sem.at[n, piece, sl],
             plane(**to), group, when)
        mine = pbuf.at[0, 0, 0] if piece == POS else other.at[piece]
        send(mine, ref_of(n, piece, sl, 1), recv_sem.at[n, piece, sl], plane(dc=1, **to), group,
             when)

    for piece in (POS, *range(PIECES)):
        send_own("up", piece, rank_of(z + 1, z, nz), 0, when=up, zz=z + 1)
        send_own("down", piece, rank_of(z - 1, z, nz), 0, when=down, zz=z - 1)
        for dx in range(1, nx):
            send_own("plane", piece, 0, slot(dx, 0), dx=dx)
        for dy in range(1, ny):
            send_own("plane", piece, 0, slot(0, dy), dy=dy)
        mine = pbuf.at[0, 0, 0] if piece == POS else other.at[piece]
        send(mine, ref_of(0, piece, 0, 1), recv_sem.at[0, piece, 0], plane(dc=1),
             (piece == POS, "chip"))
        if piece == 1:
            send(q_ref.at[:, their_cols], q_buf.at[pl.ds(rows, rows)], q_sem, plane(dc=1),
                 (False, "queries"))

    def onward(n):
        source = source_of(z, n, nz)
        there = z + jnp.where(source < z, 1, -1)
        more = jnp.logical_and(there >= 0, there < nz)
        return there, rank_of(there, source, nz), more

    def along(n, piece):
        there, n_there, more = onward(n)
        arrived_if(more, n, piece, 0)
        pass_on("along", n, piece, 0, 0, n_there, more, zz=there)

    def across(n, piece):
        _, _, more = onward(n)
        arrived_if(jnp.logical_not(more), n, piece, 0)
        if not on_line(n, piece):
            for dx in range(1, nx):
                pass_on("across", n, piece, 0, slot(dx, 0), dx=dx)
            for dy in range(1, ny):
                pass_on("across", n, piece, 0, slot(0, dy), dy=dy)

    def relay(n, piece):
        if on_line(n, piece):
            return
        for dx in range(1, nx):
            for dy in range(1, ny):
                if x_first(n, piece):
                    arrived(n, piece, slot(dx, 0))
                    pass_on("relay", n, piece, slot(dx, 0), slot(dx, dy), dy=dy)
                else:
                    arrived(n, piece, slot(0, dy))
                    pass_on("relay", n, piece, slot(0, dy), slot(dx, dy), dx=dx)

    along_x = [slot(dx, 0) for dx in range(1, nx)]
    along_y = [slot(0, dy) for dy in range(1, ny)]
    corner = [slot(dx, dy) for dx in range(1, nx) for dy in range(1, ny)]

    def farther(n):
        there, n_there, more = onward(n)
        return there, n_there, jnp.logical_and(more, n_there <= half_way)

    def values(n, slots):
        last = PIECES - 1
        for sl in slots:
            if n == 0:
                arrived(0, last, sl)
                for name, there, when in (("values up", z + 1, up), ("values down", z - 1, down)):
                    pass_on(name, 0, last, sl, sl, rank_of(there, z, nz), when, zz=there)
            elif n <= half_way:
                there, n_there, more = farther(n)
                arrived_if(more, n, last, sl)
                pass_on("values", n, last, sl, sl, n_there, more, zz=there)

    def gather(n, piece):
        for sl in ([0] if n == 0 else []) + along_x + along_y + corner:
            if on_line(n, piece):
                arrived_if(jnp.logical_not(farther(n)[2]), n, piece, sl)
            else:
                arrived(n, piece, sl)

    def positions_of(n, sl):
        return jnp.concatenate([pbuf[n, sl, 0], pbuf[n, sl, 1]], axis=1).astype(jnp.float32)

    def build_mask(n):
        mine = jnp.broadcast_to(positions_of(0, 0), (both, both))
        for sl in range(chips):
            theirs = jnp.broadcast_to(positions_of(n, sl), (both, both)).T
            mask[n, sl * both:(sl + 1) * both, :] = jnp.where(
                theirs > mine, HIDDEN, 0.0).astype(jnp.bfloat16)

    def pick(owner):
        at = lax.broadcasted_iota(jnp.int32, (rows, both), 0) + owner * rows
        return (at == lax.broadcasted_iota(jnp.int32, (rows, both), 1)).astype(jnp.bfloat16)

    picks = [pick(0), pick(1)]
    scale = math.log2(math.e) / math.sqrt(d)
    per_tile = math.gcd(max(1, 512 // rows), group)
    tile = per_tile * rows
    tiles = [(owner, t) for owner in (1, 0) for t in range(group // per_tile)]
    ones = jnp.ones((keys, d), jnp.bfloat16)

    def column(kind, t, j):
        return (kind * group + t * per_tile + j) * d

    def score(n, kind, i):
        owner, t = tiles[i]
        k_wide = jnp.concatenate([buf[n, 2 * kind].reshape(keys, d), mask[n]], axis=1)
        query = jnp.concatenate(
            [jnp.concatenate([q_buf[owner * rows:(owner + 1) * rows,
                                    column(kind, t, j):column(kind, t, j) + d], picks[owner]],
                             axis=1)
             for j in range(per_tile)], axis=0)
        return lax.dot_general(query, k_wide, (((1,), (1,)), ((), ())),
                               preferred_element_type=jnp.float32)

    def fold(n, kind, i, scores):
        owner, t = tiles[i]
        v_wide = jnp.concatenate([buf[n, 2 * kind + 1].reshape(keys, d), ones], axis=1)
        window = slice(i * tile, (i + 1) * tile)
        new_top = jnp.broadcast_to(jnp.max(scores, axis=1, keepdims=True), (tile, d))
        if n:
            old_top = top[kind, window, :]
            new_top = jnp.maximum(old_top, new_top)
            rescale = jnp.exp2((old_top - new_top) * scale)
        weights = jnp.exp2((scores - jnp.concatenate([new_top] * (keys // d), axis=1))
                           * scale).astype(jnp.bfloat16)
        got = lax.dot_general(weights, v_wide, (((1,), (0,)), ((), ())),
                              preferred_element_type=jnp.float32)
        if n:
            got = acc[kind, window, :] * jnp.concatenate([rescale, rescale], axis=1) + got
        if n < nz - 1:
            acc[kind, window, :] = got
            top[kind, window, :] = new_top
            return
        result = (got[:, :d] / got[:, d:]).astype(jnp.bfloat16)
        for j in range(per_tile):
            at = column(kind, t, j)
            if owner:
                o_buf[:, at:at + d] = result[j * rows:(j + 1) * rows, :]
            else:
                out_ref[:, pl.ds(pl.multiple_of(core * half + at, d), d)] = (
                    result[j * rows:(j + 1) * rows, :])

    wide = group * d

    def swap(kind):
        send(o_buf.at[:, pl.ds(kind * wide, wide)],
             out_ref.at[:, pl.ds(pl.multiple_of(core * half + kind * wide, wide), wide)],
             out_sem.at[kind], plane(dc=1), (False, "out", kind))

    def at(what, n, pieces):
        if n < nz and (n or what is relay):
            for piece in pieces:
                if piece == 0:
                    what(n, POS)
                what(n, piece)

    def ready(i):
        n, kind = divmod(i, 2)
        for piece in ((POS, 0, 1), (2, 3))[kind]:
            gather(n, piece)
        if kind == 0:
            build_mask(n)

    def line_values(n, slots):
        if n <= half_way:
            values(n, slots)

    def between(i):
        if i == 0:
            at(along, 3, (3,))
            at(relay, 1, (3,))
            values(0, corner)
            at(across, 3, (0, 1))
            at(relay, 2, (0, 1))
            line_values(1, along_x + along_y)
        if i == 1:
            at(across, 3, (2, 3))
            at(relay, 2, (2, 3))
            line_values(2, along_x + along_y)
            line_values(1, corner)
        if i == 2:
            at(relay, 3, (0, 1))
            line_values(2, corner)
        if i == 3:
            at(relay, 3, (2, 3))
        if i % 2:
            for what in (along, across, relay):
                at(what, i // 2 + 4, range(PIECES))

    for piece in range(PIECES):
        at(along, 1, (piece,))
        at(across, 1, (piece,))
        at(along, 2, (piece,))
        at(relay, 0, (piece,))
    for piece in range(PIECES - 1):
        at(across, 2, (piece,))
        at(along, 3, (piece,))
        at(relay, 1, (piece,))
        if piece:
            values(0, along_y if piece == 1 else along_x)
    at(across, 2, (PIECES - 1,))
    q_copy.wait()
    landed(q_buf.at[pl.ds(rows, rows)], q_sem)

    ours = len(tiles) // 2
    work = [(n, kind, i) for n in range(nz - 1) for kind in range(2) for i in range(len(tiles))]
    last = [(kind, i) for kind in range(2) for i in range(len(tiles))]
    late = [(0, len(tiles) - 1)] + [(1, i) for i in range(ours, len(tiles))]
    work += [(nz - 1,) + w for w in last if w not in late] + [(nz - 1,) + w for w in late]
    begun = 0
    ready(0)
    held = score(*work[0])
    for w, task in enumerate(work):
        following = None
        if w + 1 < len(work):
            step = 2 * work[w + 1][0] + work[w + 1][1]
            if step > begun:
                between(begun)
                begun = step
                ready(step)
                if step == 2 * nz - 1:
                    swap(0)
            if work[w + 1] == (nz - 1,) + late[1]:
                swap(1)
            following = score(*work[w + 1])
        fold(*task, held)
        held = following
    for kind in range(kinds):
        start = pl.multiple_of((1 - core) * half + kind * wide, wide)
        landed(out_ref.at[:, pl.ds(start, wide)], out_sem.at[kind])
    all_sent()


def body(query_proj, key_proj, value_proj, positions):
    rows, width = query_proj.shape
    d = HEAD_WIDTH
    heads_kv = key_proj.shape[1] // d
    group = width // d // heads_kv
    nz = lax.axis_size("outer")
    inner = lax.axis_size("inner")
    nx = 2
    ny = inner // (2 * nx)
    chips = ny * nx
    kinds = heads_kv // 2
    both = 2 * rows
    sizes = (nz, ny, nx, rows, kinds, group)
    groups = 11 + 4 * (nz - 1) + 2 * nz + min(2, nz - 1) + kinds
    hbm = pl.BlockSpec(memory_space=pltpu.HBM)
    operands = [pltpu.with_memory_space_constraint(a, pltpu.HBM) for a in (
        query_proj, key_proj, value_proj, positions.reshape(1, rows))]
    return pl.pallas_call(
        functools.partial(kernel, sizes),
        out_shape=pltpu.VMEM((rows, width), jnp.bfloat16),
        in_specs=[hbm, hbm, hbm, hbm],
        out_specs=pl.BlockSpec(memory_space=pltpu.VMEM),
        scratch_shapes=[
            pltpu.VMEM((nz, PIECES, chips, both, d), jnp.bfloat16),
            pltpu.VMEM((nz, chips, 2, 1, rows), jnp.int32),
            pltpu.VMEM((PIECES, rows, d), jnp.bfloat16),
            pltpu.VMEM((nz, chips * both, both), jnp.bfloat16),
            pltpu.VMEM((kinds, group * both, d), jnp.float32),
            pltpu.VMEM((kinds, group * both, 2 * d), jnp.float32),
            pltpu.VMEM((both, width // 2), jnp.bfloat16),
            pltpu.VMEM((rows, width // 2), jnp.bfloat16),
            pltpu.SemaphoreType.DMA((3,)),
            pltpu.SemaphoreType.DMA((nz, PIECES + 1, chips)),
            pltpu.SemaphoreType.DMA,
            pltpu.SemaphoreType.DMA((kinds,)),
            pltpu.SemaphoreType.DMA((groups,)),
        ],
        compiler_params=pltpu.CompilerParams(
            collective_id=0, has_side_effects=True, vmem_limit_bytes=48 * 1024 * 1024),
    )(*operands)


def solution(mesh):
    return jax.shard_map(
        body,
        mesh=mesh,
        in_specs=(
            P(("outer", "inner"), None),
            P(("outer", "inner"), None),
            P(("outer", "inner"), None),
            P(("outer", "inner")),
        ),
        out_specs=P(("outer", "inner"), None),
        check_vma=False,
    )
```

```python
import functools
import math

import jax
import jax.numpy as jnp
from jax import lax
from jax.experimental import pallas as pl
from jax.experimental.pallas import tpu as pltpu
from jax.sharding import PartitionSpec as P

HEAD_WIDTH = 128
HIDDEN = -1e30
PIECES = 4
POS = PIECES
MESH = pl.DeviceIdType.MESH


def rank_of(p, s, nz):
    d = jnp.abs(s - p)
    m = jnp.minimum(p, nz - 1 - p)
    return jnp.where(d <= m, 2 * d - jnp.where(s < p, 1, 0), m + d)


def source_of(p, n, nz):
    m = jnp.minimum(p, nz - 1 - p)
    near = n <= 2 * m
    d = jnp.where(near, (n + 1) // 2, n - m)
    below = jnp.where(near, n % 2, jnp.where(p > nz - 1 - p, 1, 0))
    return p + d * (1 - 2 * below)


def kernel(sizes, q_ref, k_ref, v_ref, pos_ref, out_ref, buf, pbuf, other, mask, top, acc,
           q_buf, o_buf, copy_sem, recv_sem, q_sem, out_sem, send_sem):
    nz, ny, nx, rows, kinds, group = sizes
    d = HEAD_WIDTH
    chips = ny * nx
    both = 2 * rows
    half = kinds * group * d
    z = lax.axis_index("outer")
    inner = lax.axis_index("inner")
    core = lax.rem(inner, 2)
    x = lax.rem(inner // 2, nx)
    y = inner // (2 * nx)

    def plane(dy=0, dx=0, dc=0, zz=None):
        yy = lax.rem(y + dy, ny)
        xx = lax.rem(x + dx, nx)
        cc = lax.rem(core + dc, 2)
        return (z if zz is None else zz, (yy * nx + xx) * 2 + cc)

    def slot(dx, dy):
        return dy * nx + dx

    def fetch(src, dst, n):
        c = pltpu.make_async_copy(src, dst, copy_sem.at[n])
        c.start()
        return c

    def head_cols(c, kind):
        return pl.ds(pl.multiple_of((c * kinds + kind) * d, d), d)

    for piece in range(PIECES):
        ref = v_ref if piece % 2 else k_ref
        fetch(ref.at[:, head_cols(core, piece // 2)], buf.at[0, piece, 0, pl.ds(0, rows)], 0)
        fetch(ref.at[:, head_cols(1 - core, piece // 2)], other.at[piece], 0)
    pos_copy = fetch(pos_ref, pbuf.at[0, 0, 0], 1)
    my_cols = pl.ds(pl.multiple_of(core * half, half), half)
    their_cols = pl.ds(pl.multiple_of((1 - core) * half, half), half)
    q_copy = fetch(q_ref.at[:, my_cols], q_buf.at[pl.ds(0, rows)], 2)

    up, down = z + 1 < nz, z > 0
    barrier = pltpu.get_barrier_semaphore()

    def greet(where):
        pl.semaphore_signal(barrier, inc=1, device_id=where, device_id_type=MESH)

    fixed = 1
    greet(plane(dc=1))
    for dc in range(2):
        for dx in range(1, nx):
            greet(plane(dx=dx, dc=dc))
            fixed += 1
        for dy in range(1, ny):
            greet(plane(dy=dy, dc=dc))
            fixed += 1
        pl.when(up)(functools.partial(greet, plane(dc=dc, zz=z + 1)))
        pl.when(down)(functools.partial(greet, plane(dc=dc, zz=z - 1)))
    pl.semaphore_wait(barrier, fixed + 2 * (jnp.where(up, 1, 0) + jnp.where(down, 1, 0)))
    pos_copy.wait()
    pltpu.make_async_copy(buf.at[0, :, 0], buf.at[0, :, 0], copy_sem.at[0]).wait()

    groups = {}
    waited = set()
    half_way = min(2, nz - 1)

    def on_line(n, piece):
        return piece == PIECES - 1 and 0 < n <= half_way

    def x_first(n, piece):
        return (n + piece) % 2 == 0

    def ref_of(n, piece, sl, part=None):
        if piece == POS:
            r = pbuf.at[n, sl]
            return r if part is None else r.at[part]
        r = buf.at[n, piece, sl]
        return r if part is None else r.at[pl.ds(part * rows, rows)]

    def send(src, dst, sem, to, group, when=None):
        at, cond, copies = groups.setdefault(group, (len(groups), when, []))
        c = pltpu.make_async_remote_copy(
            src_ref=src, dst_ref=dst, send_sem=send_sem.at[at], recv_sem=sem,
            device_id=to, device_id_type=MESH)
        copies.append(math.prod(src.shape))
        if when is None:
            c.start()
        else:
            pl.when(when)(c.start)

    def all_sent():
        for (is_pos, *_), (at, cond, copies) in groups.items():
            lines = sum(copies) // (rows if is_pos else rows * d)
            if is_pos:
                r = pbuf.at[0, pl.ds(0, lines // 2)] if lines > 1 else pbuf.at[0, 0, 0]
            else:
                r = q_buf.at[pl.ds(0, rows), pl.ds(0, lines * d)]
            c = pltpu.make_async_remote_copy(
                src_ref=r, dst_ref=r, send_sem=send_sem.at[at], recv_sem=q_sem,
                device_id=plane(dc=1), device_id_type=MESH)
            if cond is None:
                c.wait_send()
            else:
                pl.when(cond)(c.wait_send)

    def landed(r, sem):
        pltpu.make_async_remote_copy(
            src_ref=r, dst_ref=r, send_sem=send_sem.at[0], recv_sem=sem,
            device_id=plane(dc=1), device_id_type=MESH).wait_recv()

    def arrived(n, piece, sl):
        if (n, piece, sl) not in waited:
            waited.add((n, piece, sl))
            landed(ref_of(n, piece, sl, 1 if n == sl == 0 else None), recv_sem.at[n, piece, sl])

    def arrived_if(when, n, piece, sl):
        pl.when(when)(lambda: landed(ref_of(n, piece, sl), recv_sem.at[n, piece, sl]))

    def pass_on(name, n, piece, here, there, n_there=None, when=None, **to):
        n_there = n if n_there is None else n_there
        send(ref_of(n, piece, here), ref_of(n_there, piece, there),
             recv_sem.at[n_there, piece, there], plane(**to), (piece == POS, name, n), when)

    def send_own(name, piece, n, sl, when=None, **to):
        group = (piece == POS, name)
        send(ref_of(0, piece, 0, 0), ref_of(n, piece, sl, 0), recv_sem.at[n, piece, sl],
             plane(**to), group, when)
        mine = pbuf.at[0, 0, 0] if piece == POS else other.at[piece]
        send(mine, ref_of(n, piece, sl, 1), recv_sem.at[n, piece, sl], plane(dc=1, **to), group,
             when)

    for piece in (POS, *range(PIECES)):
        send_own("up", piece, rank_of(z + 1, z, nz), 0, when=up, zz=z + 1)
        send_own("down", piece, rank_of(z - 1, z, nz), 0, when=down, zz=z - 1)
        for dx in range(1, nx):
            send_own("plane", piece, 0, slot(dx, 0), dx=dx)
        for dy in range(1, ny):
            send_own("plane", piece, 0, slot(0, dy), dy=dy)
        mine = pbuf.at[0, 0, 0] if piece == POS else other.at[piece]
        send(mine, ref_of(0, piece, 0, 1), recv_sem.at[0, piece, 0], plane(dc=1),
             (piece == POS, "chip"))
        if piece == 1:
            send(q_ref.at[:, their_cols], q_buf.at[pl.ds(rows, rows)], q_sem, plane(dc=1),
                 (False, "queries"))

    def onward(n):
        source = source_of(z, n, nz)
        there = z + jnp.where(source < z, 1, -1)
        more = jnp.logical_and(there >= 0, there < nz)
        return there, rank_of(there, source, nz), more

    def along(n, piece):
        there, n_there, more = onward(n)
        arrived_if(more, n, piece, 0)
        pass_on("along", n, piece, 0, 0, n_there, more, zz=there)

    def across(n, piece):
        _, _, more = onward(n)
        arrived_if(jnp.logical_not(more), n, piece, 0)
        if not on_line(n, piece):
            for dx in range(1, nx):
                pass_on("across", n, piece, 0, slot(dx, 0), dx=dx)
            for dy in range(1, ny):
                pass_on("across", n, piece, 0, slot(0, dy), dy=dy)

    def relay(n, piece):
        if on_line(n, piece):
            return
        for dx in range(1, nx):
            for dy in range(1, ny):
                if x_first(n, piece):
                    arrived(n, piece, slot(dx, 0))
                    pass_on("relay", n, piece, slot(dx, 0), slot(dx, dy), dy=dy)
                else:
                    arrived(n, piece, slot(0, dy))
                    pass_on("relay", n, piece, slot(0, dy), slot(dx, dy), dx=dx)

    along_x = [slot(dx, 0) for dx in range(1, nx)]
    along_y = [slot(0, dy) for dy in range(1, ny)]
    corner = [slot(dx, dy) for dx in range(1, nx) for dy in range(1, ny)]

    def farther(n):
        there, n_there, more = onward(n)
        return there, n_there, jnp.logical_and(more, n_there <= half_way)

    def values(n, slots):
        last = PIECES - 1
        for sl in slots:
            if n == 0:
                arrived(0, last, sl)
                for name, there, when in (("values up", z + 1, up), ("values down", z - 1, down)):
                    pass_on(name, 0, last, sl, sl, rank_of(there, z, nz), when, zz=there)
            elif n <= half_way:
                there, n_there, more = farther(n)
                arrived_if(more, n, last, sl)
                pass_on("values", n, last, sl, sl, n_there, more, zz=there)

    def gather(n, piece, slots):
        for sl in slots:
            if n and not sl:
                continue
            if on_line(n, piece):
                arrived_if(jnp.logical_not(farther(n)[2]), n, piece, sl)
            else:
                arrived(n, piece, sl)

    def positions_of(n, sl):
        return jnp.concatenate([pbuf[n, sl, 0], pbuf[n, sl, 1]], axis=1).astype(jnp.float32)

    def build_mask(n, slots):
        mine = jnp.broadcast_to(positions_of(0, 0), (both, both))
        for sl in slots:
            theirs = jnp.broadcast_to(positions_of(n, sl), (both, both)).T
            mask[n, sl * both:(sl + 1) * both, :] = jnp.where(
                theirs > mine, HIDDEN, 0.0).astype(jnp.bfloat16)

    def pick(owner):
        at = lax.broadcasted_iota(jnp.int32, (rows, both), 0) + owner * rows
        return (at == lax.broadcasted_iota(jnp.int32, (rows, both), 1)).astype(jnp.bfloat16)

    picks = [pick(0), pick(1)]
    scale = math.log2(math.e) / math.sqrt(d)
    per_tile = math.gcd(max(1, 512 // rows), group)
    tile = per_tile * rows
    tiles = [(owner, t) for owner in (1, 0) for t in range(group // per_tile)]

    def column(kind, t, j):
        return (kind * group + t * per_tile + j) * d

    def score(n, kind, lo, hi, i):
        owner, t = tiles[i]
        k_wide = jnp.concatenate([buf[n, 2 * kind, lo:hi].reshape((hi - lo) * both, d),
                                  mask[n, lo * both:hi * both, :]], axis=1)
        query = jnp.concatenate(
            [jnp.concatenate([q_buf[owner * rows:(owner + 1) * rows,
                                    column(kind, t, j):column(kind, t, j) + d], picks[owner]],
                             axis=1)
             for j in range(per_tile)], axis=0)
        return lax.dot_general(query, k_wide, (((1,), (1,)), ((), ())),
                               preferred_element_type=jnp.float32)

    def fold(n, kind, lo, hi, i, scores):
        owner, t = tiles[i]
        keys = (hi - lo) * both
        later = n or lo
        v_wide = jnp.concatenate([buf[n, 2 * kind + 1, lo:hi].reshape(keys, d),
                                  jnp.ones((keys, d), jnp.bfloat16)], axis=1)
        window = slice(i * tile, (i + 1) * tile)
        new_top = jnp.broadcast_to(jnp.max(scores, axis=1, keepdims=True), (tile, d))
        if later:
            old_top = top[kind, window, :]
            new_top = jnp.maximum(old_top, new_top)
            rescale = jnp.exp2((old_top - new_top) * scale)
        weights = jnp.exp2((scores - jnp.concatenate([new_top] * (keys // d), axis=1))
                           * scale).astype(jnp.bfloat16)
        got = lax.dot_general(weights, v_wide, (((1,), (0,)), ((), ())),
                              preferred_element_type=jnp.float32)
        if later:
            got = acc[kind, window, :] * jnp.concatenate([rescale, rescale], axis=1) + got
        if n < nz - 1 or hi < chips:
            acc[kind, window, :] = got
            top[kind, window, :] = new_top
            return
        result = (got[:, :d] / got[:, d:]).astype(jnp.bfloat16)
        for j in range(per_tile):
            at = column(kind, t, j)
            if owner:
                o_buf[:, at:at + d] = result[j * rows:(j + 1) * rows, :]
            else:
                out_ref[:, pl.ds(pl.multiple_of(core * half + at, d), d)] = (
                    result[j * rows:(j + 1) * rows, :])

    wide = group * d

    def swap(kind):
        send(o_buf.at[:, pl.ds(kind * wide, wide)],
             out_ref.at[:, pl.ds(pl.multiple_of(core * half + kind * wide, wide), wide)],
             out_sem.at[kind], plane(dc=1), (False, "out", kind))

    def at(what, n, pieces):
        if n < nz and (n or what is relay):
            for piece in pieces:
                if piece == 0:
                    what(n, POS)
                what(n, piece)

    def line_values(n, slots):
        if n <= half_way:
            values(n, slots)

    def first_actions():
        for piece in range(PIECES):
            at(along, 1, (piece,))
            at(across, 1, (piece,))
            at(along, 2, (piece,))
            if piece > 1:
                at(relay, 0, (piece,))
        at(relay, 0, (1, 0))
        at(across, 2, (0,))
        values(0, along_x)

    def after(step):
        n, kind, lo, hi = step
        if n == 0 and kind == 0 and lo == 0:
            at(along, 3, (0, 1))
            at(across, 2, (1,))
            at(relay, 1, (1,))
            at(along, 3, (2,))
            at(relay, 1, (0,))
            values(0, along_y)
        elif n == 0 and lo == 0:
            at(across, 2, (2,))
            at(along, 3, (3,))
            at(across, 2, (3,))
            at(relay, 1, (2,))
            values(0, corner)
        elif n == 0 and kind == 0:
            line_values(2, along_x)
            at(across, 3, (0,))
            at(relay, 2, (1, 0))
            at(across, 3, (1,))
        elif n == 0:
            at(across, 3, (2,))
            line_values(1, along_x + along_y)
            line_values(2, along_y)
        elif n == 1 and kind == 0:
            at(relay, 2, (2,))
            line_values(2, corner)
            at(across, 3, (3,))
            line_values(1, corner)
            at(relay, 1, (3,))
            at(relay, 2, (3,))
        elif n == 1:
            at(relay, 3, (0, 1))
        elif n == 2 and kind == 0:
            at(relay, 3, (2, 3))
        if n and kind:
            for what in (along, across, relay):
                at(what, n + 3, range(PIECES))

    def ready(step):
        n, kind, lo, hi = step
        for piece in ((POS, 0, 1), (2, 3))[kind]:
            gather(n, piece, range(lo, hi))
        if kind == 0:
            build_mask(n, range(lo, hi))

    first_actions()
    q_copy.wait()
    landed(q_buf.at[pl.ds(rows, rows)], q_sem)

    steps = [(0, kind, lo, hi) for lo, hi in ((0, nx), (nx, chips)) for kind in range(2)]
    steps += [(n, kind, 0, chips) for n in range(1, nz) for kind in range(2)]
    ours = len(tiles) // 2
    work = [step + (i,) for step in steps[:-2] for i in range(len(tiles))]
    work += [step + (i,) for step in steps[-2:] for i in range(ours)]
    late = [step + (i,) for step in steps[-2:] for i in range(ours, len(tiles))]
    work += late
    begun = 0
    ready(steps[0])
    held = score(*work[0])
    for w, task in enumerate(work):
        following = None
        if w + 1 < len(work):
            step = steps.index(work[w + 1][:-1])
            if step > begun:
                after(steps[begun])
                begun = step
                ready(steps[step])
            if work[w + 1] == late[1]:
                swap(0)
                swap(1)
            following = score(*work[w + 1])
        fold(*task, held)
        held = following
    for kind in range(kinds):
        start = pl.multiple_of((1 - core) * half + kind * wide, wide)
        landed(out_ref.at[:, pl.ds(start, wide)], out_sem.at[kind])
    all_sent()


def body(query_proj, key_proj, value_proj, positions):
    rows, width = query_proj.shape
    d = HEAD_WIDTH
    heads_kv = key_proj.shape[1] // d
    group = width // d // heads_kv
    nz = lax.axis_size("outer")
    inner = lax.axis_size("inner")
    nx = 2
    ny = inner // (2 * nx)
    chips = ny * nx
    kinds = heads_kv // 2
    both = 2 * rows
    sizes = (nz, ny, nx, rows, kinds, group)
    groups = 11 + 4 * (nz - 1) + 2 * nz + min(2, nz - 1) + kinds
    hbm = pl.BlockSpec(memory_space=pltpu.HBM)
    operands = [pltpu.with_memory_space_constraint(a, pltpu.HBM) for a in (
        query_proj, key_proj, value_proj, positions.reshape(1, rows))]
    return pl.pallas_call(
        functools.partial(kernel, sizes),
        out_shape=pltpu.VMEM((rows, width), jnp.bfloat16),
        in_specs=[hbm, hbm, hbm, hbm],
        out_specs=pl.BlockSpec(memory_space=pltpu.VMEM),
        scratch_shapes=[
            pltpu.VMEM((nz, PIECES, chips, both, d), jnp.bfloat16),
            pltpu.VMEM((nz, chips, 2, 1, rows), jnp.int32),
            pltpu.VMEM((PIECES, rows, d), jnp.bfloat16),
            pltpu.VMEM((nz, chips * both, both), jnp.bfloat16),
            pltpu.VMEM((kinds, group * both, d), jnp.float32),
            pltpu.VMEM((kinds, group * both, 2 * d), jnp.float32),
            pltpu.VMEM((both, width // 2), jnp.bfloat16),
            pltpu.VMEM((rows, width // 2), jnp.bfloat16),
            pltpu.SemaphoreType.DMA((3,)),
            pltpu.SemaphoreType.DMA((nz, PIECES + 1, chips)),
            pltpu.SemaphoreType.DMA,
            pltpu.SemaphoreType.DMA((kinds,)),
            pltpu.SemaphoreType.DMA((groups,)),
        ],
        compiler_params=pltpu.CompilerParams(
            collective_id=0, has_side_effects=True, vmem_limit_bytes=48 * 1024 * 1024),
    )(*operands)


def solution(mesh):
    return jax.shard_map(
        body,
        mesh=mesh,
        in_specs=(
            P(("outer", "inner"), None),
            P(("outer", "inner"), None),
            P(("outer", "inner"), None),
            P(("outer", "inner")),
        ),
        out_specs=P(("outer", "inner"), None),
        check_vma=False,
    )
```

```python
import functools
import math

import jax
import jax.numpy as jnp
from jax import lax
from jax.experimental import pallas as pl
from jax.experimental.pallas import tpu as pltpu
from jax.sharding import PartitionSpec as P

HEAD_WIDTH = 128
HIDDEN = -1e30
PIECES = 4
POS = PIECES
MESH = pl.DeviceIdType.MESH


def rank_of(p, s, nz):
    d = jnp.abs(s - p)
    m = jnp.minimum(p, nz - 1 - p)
    return jnp.where(d <= m, 2 * d - jnp.where(s < p, 1, 0), m + d)


def source_of(p, n, nz):
    m = jnp.minimum(p, nz - 1 - p)
    near = n <= 2 * m
    d = jnp.where(near, (n + 1) // 2, n - m)
    below = jnp.where(near, n % 2, jnp.where(p > nz - 1 - p, 1, 0))
    return p + d * (1 - 2 * below)


def kernel(sizes, q_ref, k_ref, v_ref, pos_ref, out_ref, buf, pbuf, other, mask, top, acc,
           q_buf, o_buf, copy_sem, recv_sem, q_sem, out_sem, send_sem):
    nz, ny, nx, rows, kinds, group = sizes
    d = HEAD_WIDTH
    chips = ny * nx
    both = 2 * rows
    half = kinds * group * d
    z = lax.axis_index("outer")
    inner = lax.axis_index("inner")
    core = lax.rem(inner, 2)
    x = lax.rem(inner // 2, nx)
    y = inner // (2 * nx)

    def plane(dy=0, dx=0, dc=0, zz=None):
        yy = lax.rem(y + dy, ny)
        xx = lax.rem(x + dx, nx)
        cc = lax.rem(core + dc, 2)
        return (z if zz is None else zz, (yy * nx + xx) * 2 + cc)

    def slot(dx, dy):
        return dy * nx + dx

    def fetch(src, dst, n):
        c = pltpu.make_async_copy(src, dst, copy_sem.at[n])
        c.start()
        return c

    def head_cols(c, kind):
        return pl.ds(pl.multiple_of((c * kinds + kind) * d, d), d)

    for piece in range(PIECES):
        ref = v_ref if piece % 2 else k_ref
        fetch(ref.at[:, head_cols(core, piece // 2)], buf.at[0, piece, 0, pl.ds(0, rows)], 0)
        fetch(ref.at[:, head_cols(1 - core, piece // 2)], other.at[piece], 0)
    pos_copy = fetch(pos_ref, pbuf.at[0, 0, 0], 1)
    my_cols = pl.ds(pl.multiple_of(core * half, half), half)
    their_cols = pl.ds(pl.multiple_of((1 - core) * half, half), half)
    q_copy = fetch(q_ref.at[:, my_cols], q_buf.at[pl.ds(0, rows)], 2)

    up, down = z + 1 < nz, z > 0
    barrier = pltpu.get_barrier_semaphore()

    def greet(where):
        pl.semaphore_signal(barrier, inc=1, device_id=where, device_id_type=MESH)

    fixed = 1
    greet(plane(dc=1))
    for dc in range(2):
        for dx in range(1, nx):
            greet(plane(dx=dx, dc=dc))
            fixed += 1
        for dy in range(1, ny):
            greet(plane(dy=dy, dc=dc))
            fixed += 1
        pl.when(up)(functools.partial(greet, plane(dc=dc, zz=z + 1)))
        pl.when(down)(functools.partial(greet, plane(dc=dc, zz=z - 1)))
    pl.semaphore_wait(barrier, fixed + 2 * (jnp.where(up, 1, 0) + jnp.where(down, 1, 0)))
    pos_copy.wait()
    pltpu.make_async_copy(buf.at[0, :, 0], buf.at[0, :, 0], copy_sem.at[0]).wait()

    groups = {}
    waited = set()
    half_way = min(2, nz - 1)

    def on_line(n, piece):
        return piece == PIECES - 1 and 0 < n <= half_way

    def x_first(n, piece):
        return (n + piece) % 2 == 0

    def ref_of(n, piece, sl, part=None):
        if piece == POS:
            r = pbuf.at[n, sl]
            return r if part is None else r.at[part]
        r = buf.at[n, piece, sl]
        return r if part is None else r.at[pl.ds(part * rows, rows)]

    def send(src, dst, sem, to, group, when=None):
        at, cond, copies = groups.setdefault(group, (len(groups), when, []))
        c = pltpu.make_async_remote_copy(
            src_ref=src, dst_ref=dst, send_sem=send_sem.at[at], recv_sem=sem,
            device_id=to, device_id_type=MESH)
        copies.append(math.prod(src.shape))
        if when is None:
            c.start()
        else:
            pl.when(when)(c.start)

    def all_sent():
        for (is_pos, *_), (at, cond, copies) in groups.items():
            lines = sum(copies) // (rows if is_pos else rows * d)
            if is_pos:
                r = pbuf.at[0, pl.ds(0, lines // 2)] if lines > 1 else pbuf.at[0, 0, 0]
            else:
                r = q_buf.at[pl.ds(0, rows), pl.ds(0, lines * d)]
            c = pltpu.make_async_remote_copy(
                src_ref=r, dst_ref=r, send_sem=send_sem.at[at], recv_sem=q_sem,
                device_id=plane(dc=1), device_id_type=MESH)
            if cond is None:
                c.wait_send()
            else:
                pl.when(cond)(c.wait_send)

    def landed(r, sem):
        pltpu.make_async_remote_copy(
            src_ref=r, dst_ref=r, send_sem=send_sem.at[0], recv_sem=sem,
            device_id=plane(dc=1), device_id_type=MESH).wait_recv()

    def arrived(n, piece, sl):
        if (n, piece, sl) not in waited:
            waited.add((n, piece, sl))
            landed(ref_of(n, piece, sl, 1 if n == sl == 0 else None), recv_sem.at[n, piece, sl])

    def arrived_if(when, n, piece, sl):
        pl.when(when)(lambda: landed(ref_of(n, piece, sl), recv_sem.at[n, piece, sl]))

    def pass_on(name, n, piece, here, there, n_there=None, when=None, **to):
        n_there = n if n_there is None else n_there
        send(ref_of(n, piece, here), ref_of(n_there, piece, there),
             recv_sem.at[n_there, piece, there], plane(**to), (piece == POS, name, n), when)

    def send_own(name, piece, n, sl, when=None, **to):
        group = (piece == POS, name)
        send(ref_of(0, piece, 0, 0), ref_of(n, piece, sl, 0), recv_sem.at[n, piece, sl],
             plane(**to), group, when)
        mine = pbuf.at[0, 0, 0] if piece == POS else other.at[piece]
        send(mine, ref_of(n, piece, sl, 1), recv_sem.at[n, piece, sl], plane(dc=1, **to), group,
             when)

    for piece in (POS, *range(PIECES)):
        send_own("up", piece, rank_of(z + 1, z, nz), 0, when=up, zz=z + 1)
        send_own("down", piece, rank_of(z - 1, z, nz), 0, when=down, zz=z - 1)
        for dx in range(1, nx):
            send_own("plane", piece, 0, slot(dx, 0), dx=dx)
        for dy in range(1, ny):
            send_own("plane", piece, 0, slot(0, dy), dy=dy)
        mine = pbuf.at[0, 0, 0] if piece == POS else other.at[piece]
        send(mine, ref_of(0, piece, 0, 1), recv_sem.at[0, piece, 0], plane(dc=1),
             (piece == POS, "chip"))
        if piece == 1:
            send(q_ref.at[:, their_cols], q_buf.at[pl.ds(rows, rows)], q_sem, plane(dc=1),
                 (False, "queries"))

    def onward(n):
        source = source_of(z, n, nz)
        there = z + jnp.where(source < z, 1, -1)
        more = jnp.logical_and(there >= 0, there < nz)
        return there, rank_of(there, source, nz), more

    def along(n, piece):
        there, n_there, more = onward(n)
        arrived_if(more, n, piece, 0)
        pass_on("along", n, piece, 0, 0, n_there, more, zz=there)

    def across(n, piece):
        _, _, more = onward(n)
        arrived_if(jnp.logical_not(more), n, piece, 0)
        if not on_line(n, piece):
            for dx in range(1, nx):
                pass_on("across", n, piece, 0, slot(dx, 0), dx=dx)
            for dy in range(1, ny):
                pass_on("across", n, piece, 0, slot(0, dy), dy=dy)

    def relay(n, piece):
        if on_line(n, piece):
            return
        for dx in range(1, nx):
            for dy in range(1, ny):
                if x_first(n, piece):
                    arrived(n, piece, slot(dx, 0))
                    pass_on("relay", n, piece, slot(dx, 0), slot(dx, dy), dy=dy)
                else:
                    arrived(n, piece, slot(0, dy))
                    pass_on("relay", n, piece, slot(0, dy), slot(dx, dy), dx=dx)

    along_x = [slot(dx, 0) for dx in range(1, nx)]
    along_y = [slot(0, dy) for dy in range(1, ny)]
    corner = [slot(dx, dy) for dx in range(1, nx) for dy in range(1, ny)]

    def farther(n):
        there, n_there, more = onward(n)
        return there, n_there, jnp.logical_and(more, n_there <= half_way)

    def values(n, slots):
        last = PIECES - 1
        for sl in slots:
            if n == 0:
                arrived(0, last, sl)
                for name, there, when in (("values up", z + 1, up), ("values down", z - 1, down)):
                    pass_on(name, 0, last, sl, sl, rank_of(there, z, nz), when, zz=there)
            elif n <= half_way:
                there, n_there, more = farther(n)
                arrived_if(more, n, last, sl)
                pass_on("values", n, last, sl, sl, n_there, more, zz=there)

    def gather(n, piece, slots):
        for sl in slots:
            if n and not sl:
                continue
            if on_line(n, piece):
                arrived_if(jnp.logical_not(farther(n)[2]), n, piece, sl)
            else:
                arrived(n, piece, sl)

    def positions_of(n, sl):
        return jnp.concatenate([pbuf[n, sl, 0], pbuf[n, sl, 1]], axis=1).astype(jnp.float32)

    def build_mask(n, slots):
        mine = jnp.broadcast_to(positions_of(0, 0), (both, both))
        for sl in slots:
            theirs = jnp.broadcast_to(positions_of(n, sl), (both, both)).T
            mask[n, sl * both:(sl + 1) * both, :] = jnp.where(
                theirs > mine, HIDDEN, 0.0).astype(jnp.bfloat16)

    def pick(owner):
        at = lax.broadcasted_iota(jnp.int32, (rows, both), 0) + owner * rows
        return (at == lax.broadcasted_iota(jnp.int32, (rows, both), 1)).astype(jnp.bfloat16)

    picks = [pick(0), pick(1)]
    scale = math.log2(math.e) / math.sqrt(d)
    per_tile = math.gcd(max(1, 512 // rows), group)
    tile = per_tile * rows
    tiles = [(owner, t) for owner in (1, 0) for t in range(group // per_tile)]

    def column(kind, t, j):
        return (kind * group + t * per_tile + j) * d

    def score(n, kind, lo, hi, i):
        owner, t = tiles[i]
        k_wide = jnp.concatenate([buf[n, 2 * kind, lo:hi].reshape((hi - lo) * both, d),
                                  mask[n, lo * both:hi * both, :]], axis=1)
        query = jnp.concatenate(
            [jnp.concatenate([q_buf[owner * rows:(owner + 1) * rows,
                                    column(kind, t, j):column(kind, t, j) + d], picks[owner]],
                             axis=1)
             for j in range(per_tile)], axis=0)
        return lax.dot_general(query, k_wide, (((1,), (1,)), ((), ())),
                               preferred_element_type=jnp.float32)

    def fold(n, kind, lo, hi, i, scores):
        owner, t = tiles[i]
        keys = (hi - lo) * both
        later = n or lo
        v_wide = jnp.concatenate([buf[n, 2 * kind + 1, lo:hi].reshape(keys, d),
                                  jnp.ones((keys, d), jnp.bfloat16)], axis=1)
        window = slice(i * tile, (i + 1) * tile)
        new_top = jnp.broadcast_to(jnp.max(scores, axis=1, keepdims=True), (tile, d))
        if later:
            old_top = top[kind, window, :]
            new_top = jnp.maximum(old_top, new_top)
            rescale = jnp.exp2((old_top - new_top) * scale)
        weights = jnp.exp2((scores - jnp.concatenate([new_top] * (keys // d), axis=1))
                           * scale).astype(jnp.bfloat16)
        got = lax.dot_general(weights, v_wide, (((1,), (0,)), ((), ())),
                              preferred_element_type=jnp.float32)
        if later:
            got = acc[kind, window, :] * jnp.concatenate([rescale, rescale], axis=1) + got
        if n < nz - 1 or hi < chips:
            acc[kind, window, :] = got
            top[kind, window, :] = new_top
            return
        result = (got[:, :d] / got[:, d:]).astype(jnp.bfloat16)
        for j in range(per_tile):
            at = column(kind, t, j)
            if owner:
                o_buf[:, at:at + d] = result[j * rows:(j + 1) * rows, :]
            else:
                out_ref[:, pl.ds(pl.multiple_of(core * half + at, d), d)] = (
                    result[j * rows:(j + 1) * rows, :])

    wide = group * d

    def swap(kind):
        send(o_buf.at[:, pl.ds(kind * wide, wide)],
             out_ref.at[:, pl.ds(pl.multiple_of(core * half + kind * wide, wide), wide)],
             out_sem.at[kind], plane(dc=1), (False, "out", kind))

    def at(what, n, pieces):
        if n < nz and (n or what is relay):
            for piece in pieces:
                if piece == 0:
                    what(n, POS)
                what(n, piece)

    def line_values(n, slots):
        if n <= half_way:
            values(n, slots)

    def first_actions():
        for piece in range(PIECES):
            at(along, 1, (piece,))
            at(across, 1, (piece,))
            at(along, 2, (piece,))
            if piece > 1:
                at(relay, 0, (piece,))
        at(relay, 0, (1, 0))

    def after(step):
        n, kind, lo, hi = step
        if n == 0 and kind == 0 and lo == 0:
            at(across, 2, (0,))
            values(0, along_x)
            at(across, 2, (1,))
            at(along, 3, (0, 1))
            at(relay, 1, (1,))
            at(along, 3, (2,))
            at(relay, 1, (0,))
            values(0, along_y)
        elif n == 0 and lo == 0:
            at(across, 2, (2,))
            at(along, 3, (3,))
            at(across, 2, (3,))
            at(relay, 1, (2,))
            values(0, corner)
        elif n == 0 and kind == 0:
            line_values(2, along_x)
            at(across, 3, (0,))
            at(relay, 2, (1, 0))
            at(across, 3, (1,))
        elif n == 0:
            at(across, 3, (2,))
            line_values(1, along_x + along_y)
            line_values(2, along_y)
        elif n == 1 and kind == 0:
            at(relay, 2, (2,))
            line_values(2, corner)
            at(across, 3, (3,))
            line_values(1, corner)
            at(relay, 1, (3,))
            at(relay, 2, (3,))
        elif n == 1:
            at(relay, 3, (0, 1))
        elif n == 2 and kind == 0:
            at(relay, 3, (2, 3))
        if n and kind:
            for what in (along, across, relay):
                at(what, n + 3, range(PIECES))

    def ready(step):
        n, kind, lo, hi = step
        for piece in ((POS, 0, 1), (2, 3))[kind]:
            gather(n, piece, range(lo, hi))
        if kind == 0:
            build_mask(n, range(lo, hi))

    first_actions()
    q_copy.wait()
    landed(q_buf.at[pl.ds(rows, rows)], q_sem)

    steps = [(0, kind, lo, hi) for lo, hi in ((0, nx), (nx, chips)) for kind in range(2)]
    steps += [(n, kind, 0, chips) for n in range(1, nz) for kind in range(2)]
    ours = len(tiles) // 2
    work = [step + (i,) for step in steps[:-2] for i in range(len(tiles))]
    work += [step + (i,) for step in steps[-2:] for i in range(ours)]
    late = [step + (i,) for step in steps[-2:] for i in range(ours, len(tiles))]
    work += late
    begun = 0
    ready(steps[0])
    held = score(*work[0])
    for w, task in enumerate(work):
        following = None
        if w + 1 < len(work):
            step = steps.index(work[w + 1][:-1])
            if step > begun:
                after(steps[begun])
                begun = step
                ready(steps[step])
            if work[w + 1] == late[1]:
                swap(0)
                swap(1)
            following = score(*work[w + 1])
        fold(*task, held)
        held = following
    for kind in range(kinds):
        start = pl.multiple_of((1 - core) * half + kind * wide, wide)
        landed(out_ref.at[:, pl.ds(start, wide)], out_sem.at[kind])
    all_sent()


def body(query_proj, key_proj, value_proj, positions):
    rows, width = query_proj.shape
    d = HEAD_WIDTH
    heads_kv = key_proj.shape[1] // d
    group = width // d // heads_kv
    nz = lax.axis_size("outer")
    inner = lax.axis_size("inner")
    nx = 2
    ny = inner // (2 * nx)
    chips = ny * nx
    kinds = heads_kv // 2
    both = 2 * rows
    sizes = (nz, ny, nx, rows, kinds, group)
    groups = 11 + 4 * (nz - 1) + 2 * nz + min(2, nz - 1) + kinds
    hbm = pl.BlockSpec(memory_space=pltpu.HBM)
    operands = [pltpu.with_memory_space_constraint(a, pltpu.HBM) for a in (
        query_proj, key_proj, value_proj, positions.reshape(1, rows))]
    return pl.pallas_call(
        functools.partial(kernel, sizes),
        out_shape=pltpu.VMEM((rows, width), jnp.bfloat16),
        in_specs=[hbm, hbm, hbm, hbm],
        out_specs=pl.BlockSpec(memory_space=pltpu.VMEM),
        scratch_shapes=[
            pltpu.VMEM((nz, PIECES, chips, both, d), jnp.bfloat16),
            pltpu.VMEM((nz, chips, 2, 1, rows), jnp.int32),
            pltpu.VMEM((PIECES, rows, d), jnp.bfloat16),
            pltpu.VMEM((nz, chips * both, both), jnp.bfloat16),
            pltpu.VMEM((kinds, group * both, d), jnp.float32),
            pltpu.VMEM((kinds, group * both, 2 * d), jnp.float32),
            pltpu.VMEM((both, width // 2), jnp.bfloat16),
            pltpu.VMEM((rows, width // 2), jnp.bfloat16),
            pltpu.SemaphoreType.DMA((3,)),
            pltpu.SemaphoreType.DMA((nz, PIECES + 1, chips)),
            pltpu.SemaphoreType.DMA,
            pltpu.SemaphoreType.DMA((kinds,)),
            pltpu.SemaphoreType.DMA((groups,)),
        ],
        compiler_params=pltpu.CompilerParams(
            collective_id=0, has_side_effects=True, vmem_limit_bytes=48 * 1024 * 1024),
    )(*operands)


def solution(mesh):
    return jax.shard_map(
        body,
        mesh=mesh,
        in_specs=(
            P(("outer", "inner"), None),
            P(("outer", "inner"), None),
            P(("outer", "inner"), None),
            P(("outer", "inner")),
        ),
        out_specs=P(("outer", "inner"), None),
        check_vma=False,
    )
```
